64 devices in a mesh: dp: 4 (over x, y), tp: 16 (over z, core).
Axes of the slice: x: 2, y: 2, z: 8, core: 2. Of those that a mesh axis runs over, the one named last changes fastest.
The devices are a block of a 4x4x8 slice.
Arguments:
- x_in: bfloat16 [4096, 8192], P('dp'), parts along dimension 0
- g_norm: bfloat16 [8192], replicated
- w_q: bfloat16 [8192, 8192], P(None, 'tp')
- w_k: bfloat16 [8192, 1024], replicated
- w_v: bfloat16 [8192, 1024], replicated
- w_o: bfloat16 [8192, 8192], P('tp')
- w_gate: bfloat16 [8192, 22016], P(None, 'tp')
- w_up: bfloat16 [8192, 22016], P(None, 'tp')
- w_down: bfloat16 [22016, 8192], P('tp')
Outputs:
- output 1: bfloat16 [4096, 8192], P('dp'), parts along dimension 0
- output 2: bfloat16 [4096, 16, 128], P('dp', 'tp'), parts along dimension 0
- output 3: bfloat16 [4096, 16, 128], P('dp', 'tp'), parts along dimension 0
There are 4 independent parts. The reference program is written for one: setup_inputs(seed, part) draws one part's arguments, and reference() takes and returns one part's arrays. A program takes and returns all parts, laid end to end along the dimension named above; an argument that names none is the same for every part.
All inputs are finite; a program needn't handle non-finite values.
Results may differ from the reference program's by a relative error of at most 0.0157075.
Values are sent between devices in bfloat16 or wider.
A program may use at most 768 MiB of HBM per device.

```python
import math
import jax
import jax.numpy as jnp
from jax import lax

TOKENS = 1024
D = 8192
HEADS = 64
KV_HEADS = 8
HEAD = 128
FF = 22016
KV_SLOTS = 16
QBLOCK = 128

ROPE_BASE = 500000.0
NORM_EPS = 1e-5


def setup_inputs(seed: int = 0, part: int = 0) -> dict:
    key_list = jax.random.split(jax.random.key(seed), 10)
    part_key = jax.random.fold_in(key_list[9], part)
    q_gain = math.sqrt(math.log(TOKENS / 16.0)) / 1.09
    x_val = 0.7 * jax.random.normal(part_key, (TOKENS, D), jnp.float32)
    g_val = jnp.exp(0.7 * jax.random.normal(key_list[0], (D,), jnp.float32) - 0.49)
    w_q = jax.random.normal(key_list[1], (D, HEADS * HEAD), jnp.float32) * (q_gain / math.sqrt(D))
    w_k = jax.random.normal(key_list[2], (D, KV_HEADS * HEAD), jnp.float32) / math.sqrt(D)
    w_v = jax.random.normal(key_list[3], (D, KV_HEADS * HEAD), jnp.float32) / math.sqrt(D)
    w_o = jax.random.normal(key_list[4], (HEADS * HEAD, D), jnp.float32) * (3.0 / math.sqrt(HEADS * HEAD))
    w_gate = jax.random.normal(key_list[5], (D, FF), jnp.float32) / math.sqrt(D)
    w_up = jax.random.normal(key_list[6], (D, FF), jnp.float32) / math.sqrt(D)
    w_down = jax.random.normal(key_list[7], (FF, D), jnp.float32) / math.sqrt(FF)
    return {'x_in': x_val.astype(jnp.bfloat16), 'g_norm': g_val.astype(jnp.bfloat16), 'w_q': w_q.astype(jnp.bfloat16), 'w_k': w_k.astype(jnp.bfloat16), 'w_v': w_v.astype(jnp.bfloat16), 'w_o': w_o.astype(jnp.bfloat16), 'w_gate': w_gate.astype(jnp.bfloat16), 'w_up': w_up.astype(jnp.bfloat16), 'w_down': w_down.astype(jnp.bfloat16)}


def rope_tables(positions):
    inv_freq = ROPE_BASE ** (-jnp.arange(0, HEAD, 2, dtype=jnp.float32) / HEAD)
    angles = positions.astype(jnp.float32)[:, None] * inv_freq[None, :]
    return jnp.cos(angles), jnp.sin(angles)


def apply_rope(projected, cos_tab, sin_tab):
    half_dim = HEAD // 2
    lower_half = projected[..., :half_dim]
    upper_half = projected[..., half_dim:]
    cos_b = cos_tab[:, None, :]
    sin_b = sin_tab[:, None, :]
    return jnp.concatenate([lower_half * cos_b - upper_half * sin_b, upper_half * cos_b + lower_half * sin_b], axis=-1)


def reference(x_in, g_norm, w_q, w_k, w_v, w_o, w_gate, w_up, w_down):
    x_f32 = x_in.astype(jnp.float32)
    inv_rms = lax.rsqrt(jnp.mean(x_f32 * x_f32, axis=-1, keepdims=True) + NORM_EPS)
    normed = (x_f32 * inv_rms * g_norm.astype(jnp.float32)).astype(jnp.bfloat16)
    cos_tab, sin_tab = rope_tables(jnp.arange(TOKENS))
    q_proj = jnp.dot(normed, w_q, preferred_element_type=jnp.float32).reshape(TOKENS, HEADS, HEAD)
    k_proj = jnp.dot(normed, w_k, preferred_element_type=jnp.float32).reshape(TOKENS, KV_HEADS, HEAD)
    q_rot = apply_rope(q_proj, cos_tab, sin_tab).astype(jnp.bfloat16)
    k_rot = apply_rope(k_proj, cos_tab, sin_tab).astype(jnp.bfloat16)
    v_proj = jnp.dot(normed, w_v, preferred_element_type=jnp.float32).astype(jnp.bfloat16).reshape(TOKENS, KV_HEADS, HEAD)
    group_size = HEADS // KV_HEADS
    q_grouped = q_rot.reshape(TOKENS, KV_HEADS, group_size, HEAD)
    k_f32 = k_rot.astype(jnp.float32)
    v_f32 = v_proj.astype(jnp.float32)
    score_scale = 1.0 / math.sqrt(HEAD)
    key_pos = jnp.arange(TOKENS)

    def attend_block(block_idx):
        row_start = block_idx * QBLOCK
        q_part = lax.dynamic_slice_in_dim(q_grouped, row_start, QBLOCK, axis=0).astype(jnp.float32)
        scores = jnp.einsum('qgrd,kgd->grqk', q_part, k_f32) * score_scale
        query_pos = row_start + jnp.arange(QBLOCK)
        visible = key_pos[None, :] <= query_pos[:, None]
        scores = jnp.where(visible, scores, -1e30)
        probs = jax.nn.softmax(scores, axis=-1).astype(jnp.bfloat16).astype(jnp.float32)
        return jnp.einsum('grqk,kgd->qgrd', probs, v_f32).astype(jnp.bfloat16)

    attn_blocks = lax.map(attend_block, jnp.arange(TOKENS // QBLOCK))
    attn_out = attn_blocks.reshape(TOKENS, HEADS * HEAD)
    attn_sum = jnp.dot(attn_out, w_o, preferred_element_type=jnp.float32)
    gate_proj = jnp.dot(normed, w_gate, preferred_element_type=jnp.float32)
    up_proj = jnp.dot(normed, w_up, preferred_element_type=jnp.float32)
    hidden = (jax.nn.silu(gate_proj) * up_proj).astype(jnp.bfloat16)
    mlp_sum = jnp.dot(hidden, w_down, preferred_element_type=jnp.float32)
    y_out = (x_f32 + attn_sum + mlp_sum).astype(jnp.bfloat16)
    slot_repeat = KV_SLOTS // KV_HEADS
    k_cache = jnp.repeat(k_rot, slot_repeat, axis=1)
    v_cache = jnp.repeat(v_proj, slot_repeat, axis=1)
    return (y_out, k_cache, v_cache)
```

```python
import functools
import math
import jax
import jax.numpy as jnp
from jax import lax
from jax.experimental import pallas as pl
from jax.experimental.pallas import tpu as pltpu
from jax.sharding import PartitionSpec as P

HEAD_DIM = 128
ROPE_BASE = 500000.0
NORM_EPS = 1e-5

ROW_BLOCKS = 4
K_STEPS = 16
N_STEPS = 8
SUBS = 4
MESH = pl.DeviceIdType.MESH


def rope_tables(positions):
    inv_freq = ROPE_BASE ** (-jnp.arange(0, HEAD_DIM, 2, dtype=jnp.float32) / HEAD_DIM)
    angles = positions.astype(jnp.float32)[:, None] * inv_freq[None, :]
    return jnp.cos(angles), jnp.sin(angles)


def round_up(n, m):
    return (n + m - 1) // m * m


def layer_kernel(cfg, x_hbm, g_ref, cos_ref, sin_ref, wq_hbm, wk_hbm, wv_hbm, wo_hbm, wg_hbm, wu_hbm, wd_hbm,
                 y_hbm, k_hbm, v_hbm,
                 xbuf, a_buf, wgu, wqkv, wo_buf, wd_buf, acc_gu, acc_qkv, m_buf, o_buf, q_buf, k_buf, v_buf,
                 pbuf, precv, rsbuf, ybuf, xown,
                 x_sem, wk_sem, wn_sem, kv_sem, xown_sem, ps_send, ps_recv, rs_send, rs_recv, ag_send, ag_recv,
                 yl_sem, yp_send, yp_recv, credit):
    tokens, width, ff, fpad, q_cols, kv_heads, tp_size = cfg
    blocks = ROW_BLOCKS
    rows = tokens // blocks
    ring = tp_size // 2
    k_w = width // K_STEPS
    n_w = width // N_STEPS
    half = width // 2
    c_w = half // (2 * ring)
    per_n = n_w // c_w
    s_rows = rows // SUBS
    q_local = q_cols // HEAD_DIM
    scale = 1.0 / math.sqrt(HEAD_DIM)
    f32, bf16 = jnp.float32, jnp.bfloat16

    me = lax.axis_index('tp')
    pos, core = me // 2, me % 2
    nxt = (lax.rem(pos + 1, ring) * 2 + core, lax.rem(pos + ring - 1, ring) * 2 + core)
    partner = pos * 2 + (1 - core)
    head_col = pl.multiple_of(me * kv_heads // tp_size * HEAD_DIM, HEAD_DIM)

    barrier = pltpu.get_barrier_semaphore()
    for other in (nxt[0], nxt[1], partner):
        pl.semaphore_signal(barrier, inc=1, device_id={'tp': other}, device_id_type=MESH)
    pl.semaphore_wait(barrier, 3)

    def x_copy(b):
        return pltpu.make_async_copy(x_hbm.at[pl.ds(pl.multiple_of(b * rows, rows), rows)], xbuf, x_sem)

    def k_copies(k):
        s = lax.rem(k, 3)
        lo = pl.multiple_of(k * k_w, k_w)
        return (
            pltpu.make_async_copy(wg_hbm.at[:, pl.ds(lo, k_w)], wgu.at[s, pl.ds(0, ff)], wk_sem.at[s, 0]),
            pltpu.make_async_copy(wu_hbm.at[:, pl.ds(lo, k_w)], wgu.at[s, pl.ds(fpad, ff)], wk_sem.at[s, 1]),
            pltpu.make_async_copy(wq_hbm.at[pl.ds(lo, k_w)], wqkv.at[s, :, pl.ds(0, q_cols)], wk_sem.at[s, 2]),
            pltpu.make_async_copy(wk_hbm.at[pl.ds(lo, k_w), pl.ds(head_col, HEAD_DIM)],
                                  wqkv.at[s, :, pl.ds(q_cols, HEAD_DIM)], wk_sem.at[s, 3]),
            pltpu.make_async_copy(wv_hbm.at[pl.ds(lo, k_w), pl.ds(head_col, HEAD_DIM)],
                                  wqkv.at[s, :, pl.ds(q_cols + HEAD_DIM, HEAD_DIM)], wk_sem.at[s, 4]),
        )

    def n_copies(n):
        s = lax.rem(n, 3)
        piece = n // (N_STEPS // 2)
        side = jnp.where(piece == 0, 1 - core, core)
        lo = pl.multiple_of(side * half + lax.rem(n, N_STEPS // 2) * n_w, n_w)
        return (
            pltpu.make_async_copy(wo_hbm.at[:, pl.ds(lo, n_w)], wo_buf.at[s], wn_sem.at[s, 0]),
            pltpu.make_async_copy(wd_hbm.at[:, pl.ds(lo, n_w)], wd_buf.at[s, pl.ds(0, ff)], wn_sem.at[s, 1]),
        )

    def start(copies):
        for copy in copies:
            copy.start()

    def wait(copies):
        for copy in copies:
            copy.wait()

    def kv_copies(b):
        r = pl.ds(pl.multiple_of(b * rows, rows), rows)
        return (pltpu.make_async_copy(k_buf.at[r], k_hbm.at[r], kv_sem.at[0]),
                pltpu.make_async_copy(v_buf.at[r], v_hbm.at[r], kv_sem.at[1]))

    def xown_copies(b):
        out = []
        for d in range(2):
            col = pl.multiple_of(core * half + (d * ring + pos) * c_w, c_w)
            out.append(pltpu.make_async_copy(
                x_hbm.at[pl.ds(pl.multiple_of(b * rows, rows), rows), pl.ds(col, c_w)],
                xown.at[lax.rem(b, 2), d], xown_sem.at[lax.rem(b, 2), d]))
        return out

    def ps_copy(b, n):
        part = pl.ds(n * per_n, per_n)
        return pltpu.make_async_remote_copy(
            pbuf.at[0, part], precv.at[lax.rem(b, 2), part], ps_send, ps_recv.at[lax.rem(b, 2)],
            device_id={'tp': partner}, device_id_type=MESH)

    def rs_copy(src, b, d, s, sub):
        par = lax.rem(b, 2)
        return pltpu.make_async_remote_copy(
            src, rsbuf.at[par, d, s, sub], rs_send, rs_recv.at[par, d, s, sub],
            device_id={'tp': nxt[d]}, device_id_type=MESH)

    def ag_copy(b, d, s, k, sub):
        ref = ybuf.at[b, d * ring + k, sub]
        return pltpu.make_async_remote_copy(
            ref, ref, ag_send.at[b], ag_recv.at[b, d, s, sub], device_id={'tp': nxt[d]}, device_id_type=MESH)

    def put_out(b, d, k, sub):
        src = ybuf.at[b, d * ring + k, sub]
        r = pl.multiple_of(b * rows + sub * s_rows, s_rows)
        col = pl.multiple_of(core * half + (d * ring + k) * c_w, c_w)
        dst = y_hbm.at[pl.ds(r, s_rows), pl.ds(col, c_w)]
        pltpu.make_async_copy(src, dst, yl_sem.at[b]).start()
        pltpu.make_async_remote_copy(src, dst, yp_send.at[b], yp_recv.at[b],
                                     device_id={'tp': partner}, device_id_type=MESH).start()

    def own_share(b, d, k, sub):
        par = lax.rem(b, 2)
        q = d * ring + k
        return pbuf[1 + par, q, sub].astype(f32) + precv[par, q, sub].astype(f32)

    def rs_step(b, s, sub):
        par = lax.rem(b, 2)
        for d in range(2):
            k = lax.rem(pos + 2 * ring - 1 - s, ring) if d == 0 else lax.rem(pos + 1 + s, ring)

            @pl.when(s == 0)
            def _():
                src = pbuf.at[1 + par, d * ring + k, sub]
                src[...] = own_share(b, d, k, sub).astype(bf16)
                rs_copy(src, b, d, s, sub).start()

            @pl.when(s > 0)
            def _():
                src = rsbuf.at[par, d, s - 1, sub]
                rs_copy(src, b, d, s - 1, sub).wait_recv()
                src[...] = (own_share(b, d, k, sub) + src[...].astype(f32)).astype(bf16)
                rs_copy(src, b, d, s, sub).start()

    def ag_step(b, s, sub):
        par = lax.rem(b, 2)

        @pl.when((s == 0) & (sub == 0))
        def _():
            wait(xown_copies(b))

        for d in range(2):
            k = lax.rem(pos + ring - s, ring) if d == 0 else lax.rem(pos + s, ring)

            @pl.when(s == 0)
            def _():
                last = rsbuf.at[par, d, ring - 2, sub]
                rs_copy(last, b, d, ring - 2, sub).wait_recv()
                total = own_share(b, d, k, sub) + last[...].astype(f32)
                r = pl.ds(pl.multiple_of(sub * s_rows, s_rows), s_rows)
                ybuf[b, d * ring + k, sub] = (xown[par, d, r].astype(f32) + total).astype(bf16)

            @pl.when(s > 0)
            def _():
                ag_copy(b, d, s - 1, k, sub).wait_recv()

            ag_copy(b, d, s, k, sub).start()
            put_out(b, d, k, sub)

    def ag_last(b, sub):
        for d in range(2):
            k = lax.rem(pos + 1, ring) if d == 0 else lax.rem(pos + ring - 1, ring)
            ag_copy(b, d, ring - 2, k, sub).wait_recv()
            put_out(b, d, k, sub)

    def comm(t, j):
        s, sub = j // SUBS, lax.rem(j, SUBS)

        @pl.when((s == 0) & (t >= 3))
        def _():
            ag_last(t - 3, sub)

        @pl.when((t >= 1) & (t <= blocks))
        def _():
            rs_step(t - 1, s, sub)

        @pl.when((t >= 2) & (t <= blocks + 1))
        def _():
            ag_step(t - 2, s, sub)

        @pl.when((j == SUBS) & (t >= 2) & (t < blocks))
        def _():
            pl.semaphore_signal(credit, inc=1, device_id={'tp': partner}, device_id_type=MESH)

    def norm_rows(i, carry):
        r = pl.ds(pl.multiple_of(i * 16, 16), 16)
        x32 = xbuf[r].astype(f32)
        inv = lax.rsqrt(jnp.mean(x32 * x32, axis=-1, keepdims=True) + NORM_EPS)
        a_buf[r] = (x32 * inv * g_ref[...].astype(f32)).astype(bf16)
        return carry

    def k_step(k):
        s = lax.rem(k, 3)
        wait(k_copies(k))

        @pl.when(k + 2 < K_STEPS)
        def _():
            start(k_copies(k + 2))

        @pl.when(k + 2 >= K_STEPS)
        def _():
            start(n_copies(k + 2 - K_STEPS))

        a_k = a_buf[:, pl.ds(pl.multiple_of(k * k_w, k_w), k_w)]
        for lo in range(0, 2 * fpad, 512):
            hi = min(lo + 512, 2 * fpad)
            acc_gu[:, lo:hi] += lax.dot_general(a_k, wgu[s, lo:hi], (((1,), (1,)), ((), ())), preferred_element_type=f32)
        acc_qkv[...] += jnp.dot(a_k, wqkv[s], preferred_element_type=f32)

    def rope(v, t):
        r = pl.ds(pl.multiple_of(t * rows, rows), rows)
        return v * cos_ref[r] + pltpu.roll(v, HEAD_DIM // 2, 1) * sin_ref[r]

    def attend(t, h):
        r = pl.ds(pl.multiple_of(t * rows, rows), rows)
        if h == 0:
            k_buf[r] = rope(acc_qkv[:, q_cols:q_cols + HEAD_DIM], t).astype(bf16)
            v_buf[r] = acc_qkv[:, q_cols + HEAD_DIM:q_cols + 2 * HEAD_DIM].astype(bf16)
            start(kv_copies(t))
            start(n_copies(2))
        span = slice(h * HEAD_DIM, (h + 1) * HEAD_DIM)
        q_rot = rope(acc_qkv[:, span], t).astype(bf16)
        scores = lax.dot_general(q_rot, k_buf[...], (((1,), (1,)), ((), ())), preferred_element_type=f32) * scale
        row_id = t * rows + lax.broadcasted_iota(jnp.int32, scores.shape, 0)
        col_id = lax.broadcasted_iota(jnp.int32, scores.shape, 1)
        scores = jnp.where(col_id <= row_id, scores, -1e30)
        expd = jnp.exp(scores - jnp.max(scores, axis=-1, keepdims=True))
        probs = (expd / jnp.sum(expd, axis=-1, keepdims=True)).astype(bf16)
        o_buf[:, span] = jnp.dot(probs, v_buf[...], preferred_element_type=f32).astype(bf16)
        q_rows = rows // q_local
        part = slice(h * q_rows, (h + 1) * q_rows)
        gate = acc_gu[part, 0:fpad]
        m_buf[part] = (gate * (1.0 / (1.0 + jnp.exp(-gate))) * acc_gu[part, fpad:2 * fpad]).astype(bf16)

    def n_step(t, n):
        s = lax.rem(n, 3)
        wait(n_copies(n))

        @pl.when((n >= 1) & (n + 2 < N_STEPS))
        def _():
            start(n_copies(n + 2))

        @pl.when((n + 2 >= N_STEPS) & (t + 1 < blocks))
        def _():
            start(k_copies(n + 2 - N_STEPS))

        @pl.when((n == 0) & (t >= 2))
        def _():
            pl.semaphore_wait(credit, 1)

        mine = n >= N_STEPS // 2
        slot = jnp.where(mine, 1 + lax.rem(t, 2), 0)
        piece = lax.rem(n, N_STEPS // 2)
        o_v, m_v = o_buf[...], m_buf[...]
        for i in range(per_n):
            cols = slice(i * c_w, (i + 1) * c_w)
            out = (jnp.dot(o_v, wo_buf[s, :, cols], preferred_element_type=f32)
                   + jnp.dot(m_v, wd_buf[s, :, cols], preferred_element_type=f32)).astype(bf16)
            pbuf[slot, piece * per_n + i] = out.reshape(SUBS, s_rows, c_w)

        @pl.when(jnp.logical_not(mine))
        def _():
            ps_copy(t, piece).start()

    x_copy(0).start()
    start(k_copies(0))
    start(k_copies(1))
    wgu[:, ff:fpad] = jnp.zeros((3, fpad - ff, k_w), bf16)
    wgu[:, fpad + ff:] = jnp.zeros((3, fpad - ff, k_w), bf16)
    wd_buf[:, ff:] = jnp.zeros((3, fpad - ff, n_w), bf16)
    k_buf[...] = jnp.zeros(k_buf.shape, bf16)
    v_buf[...] = jnp.zeros(v_buf.shape, bf16)

    def slot_body(t, carry):
        computes = t < blocks
        sends = (t >= 1) & (t <= blocks)

        @pl.when(sends)
        def _():
            pltpu.make_async_copy(precv.at[lax.rem(t - 1, 2)], precv.at[lax.rem(t - 1, 2)],
                                  ps_recv.at[lax.rem(t - 1, 2)]).wait()
            start(xown_copies(t - 1))

        @pl.when(computes)
        def _():
            x_copy(t).wait()
            lax.fori_loop(0, rows // 16, norm_rows, 0)

            @pl.when(t + 1 < blocks)
            def _():
                x_copy(t + 1).start()

            acc_gu[...] = jnp.zeros(acc_gu.shape, f32)
            acc_qkv[...] = jnp.zeros(acc_qkv.shape, f32)

        def k_body(k, c):
            comm(t, k)

            @pl.when(computes)
            def _():
                k_step(k)
            return c

        lax.fori_loop(0, K_STEPS, k_body, 0)
        for h in range(q_local):
            comm(t, K_STEPS + h)

            @pl.when(computes)
            def _():
                attend(t, h)

        def n_body(n, c):
            comm(t, K_STEPS + q_local + n)

            @pl.when(computes)
            def _():
                n_step(t, n)
            return c

        lax.fori_loop(0, N_STEPS, n_body, 0)

        @pl.when(sends)
        def _():
            pltpu.make_async_copy(rsbuf.at[0], rsbuf.at[0], rs_send).wait()

        @pl.when(computes)
        def _():
            pltpu.make_async_copy(pbuf.at[0], pbuf.at[0], ps_send).wait()
            wait(kv_copies(t))
        return carry

    lax.fori_loop(0, blocks + 2, slot_body, 0)
    for sub in range(SUBS):
        ag_last(blocks - 1, sub)
    for b in range(blocks):
        whole, sent = ybuf.at[b], ybuf.at[b, pl.ds(0, 2 * (ring - 1))]
        pltpu.make_async_copy(sent, sent, ag_send.at[b]).wait()
        for sem in (yl_sem, yp_send, yp_recv):
            pltpu.make_async_copy(whole, whole, sem.at[b]).wait()


def solution(mesh):
    tp_size = mesh.shape['tp']

    def local_layer(x_in, g_norm, w_q, w_k, w_v, w_o, w_gate, w_up, w_down):
        tokens, width = x_in.shape
        ff, q_cols = w_gate.shape[1], w_q.shape[1]
        kv_heads = w_k.shape[1] // HEAD_DIM
        fpad = round_up(ff, HEAD_DIM)
        rows, ring = tokens // ROW_BLOCKS, tp_size // 2
        k_w, n_w = width // K_STEPS, width // N_STEPS
        c_w = width // (4 * ring)
        s_rows = rows // SUBS
        assert K_STEPS + q_cols // HEAD_DIM + N_STEPS == SUBS * (ring - 1)
        cos_tab, sin_tab = rope_tables(jnp.arange(tokens))
        cos_full = jnp.concatenate([cos_tab, cos_tab], axis=1)
        sin_full = jnp.concatenate([-sin_tab, sin_tab], axis=1)
        cfg = (tokens, width, ff, fpad, q_cols, kv_heads, tp_size)
        bf16, f32 = jnp.bfloat16, jnp.float32
        dma, vmem = pltpu.SemaphoreType.DMA, pltpu.VMEM
        any_spec, vmem_spec = pl.BlockSpec(memory_space=pl.ANY), pl.BlockSpec(memory_space=pltpu.VMEM)
        blocks = ROW_BLOCKS
        y_out, k_out, v_out = pl.pallas_call(
            functools.partial(layer_kernel, cfg),
            out_shape=(jax.ShapeDtypeStruct((tokens, width), bf16),
                       jax.ShapeDtypeStruct((tokens, HEAD_DIM), bf16),
                       jax.ShapeDtypeStruct((tokens, HEAD_DIM), bf16)),
            in_specs=[any_spec, vmem_spec, vmem_spec, vmem_spec] + [any_spec] * 7,
            out_specs=(any_spec,) * 3,
            scratch_shapes=[
                vmem((rows, width), bf16),
                vmem((rows, width), bf16),
                vmem((3, 2 * fpad, k_w), bf16),
                vmem((3, k_w, q_cols + 2 * HEAD_DIM), bf16),
                vmem((3, q_cols, n_w), bf16),
                vmem((3, fpad, n_w), bf16),
                vmem((rows, 2 * fpad), f32),
                vmem((rows, q_cols + 2 * HEAD_DIM), f32),
                vmem((rows, fpad), bf16),
                vmem((rows, q_cols), bf16),
                vmem((rows, HEAD_DIM), bf16),
                vmem((tokens, HEAD_DIM), bf16),
                vmem((tokens, HEAD_DIM), bf16),
                vmem((3, 2 * ring, SUBS, s_rows, c_w), bf16),
                vmem((2, 2 * ring, SUBS, s_rows, c_w), bf16),
                vmem((2, 2, ring - 1, SUBS, s_rows, c_w), bf16),
                vmem((blocks, 2 * ring, SUBS, s_rows, c_w), bf16),
                vmem((2, 2, rows, c_w), bf16),
                dma, dma((3, 5)), dma((3, 2)), dma((2,)), dma((2, 2)),
                dma, dma((2,)), dma, dma((2, 2, ring - 1, SUBS)),
                dma((blocks,)), dma((blocks, 2, ring - 1, SUBS)),
                dma((blocks,)), dma((blocks,)), dma((blocks,)),
                pltpu.SemaphoreType.REGULAR,
            ],
            compiler_params=pltpu.CompilerParams(collective_id=0, has_side_effects=True, vmem_limit_bytes=67043328),
        )(x_in, g_norm.reshape(1, width), cos_full, sin_full, w_q, w_k, w_v, w_o, w_gate.T, w_up.T, w_down)
        return y_out, k_out.reshape(tokens, 1, HEAD_DIM), v_out.reshape(tokens, 1, HEAD_DIM)

    return jax.shard_map(local_layer, mesh=mesh, in_specs=(P('dp', None), P(None), P(None, 'tp'), P(None, None), P(None, None), P('tp', None), P(None, 'tp'), P(None, 'tp'), P('tp', None)), out_specs=(P('dp', None), P('dp', 'tp', None), P('dp', 'tp', None)), check_vma=False)
```

```python
import functools
import math
import jax
import jax.numpy as jnp
import numpy as np
from jax import lax
from jax.experimental import pallas as pl
from jax.experimental.pallas import tpu as pltpu
from jax.sharding import PartitionSpec as P

HEAD_DIM = 128
ROPE_BASE = 500000.0
NORM_EPS = 1e-5

ROW_BLOCKS = 4
K_STEPS = 16
N_STEPS = 8
SUBS = 4
MESH = pl.DeviceIdType.MESH


def rope_tables(tokens):
    inv_freq = np.float32(ROPE_BASE) ** (-np.arange(0, HEAD_DIM, 2, dtype=np.float32) / np.float32(HEAD_DIM))
    angles = (np.arange(tokens, dtype=np.float32)[:, None] * inv_freq[None, :].astype(np.float32)).astype(np.float64)
    cos_tab, sin_tab = np.cos(angles).astype(np.float32), np.sin(angles).astype(np.float32)
    return np.concatenate([cos_tab, cos_tab], axis=1), np.concatenate([-sin_tab, sin_tab], axis=1)


def round_up(n, m):
    return (n + m - 1) // m * m


def layer_kernel(cfg, x_hbm, g_ref, cos_ref, sin_ref, wq_hbm, wk_hbm, wv_hbm, wo_hbm, wg_hbm, wu_hbm, wd_hbm,
                 y_hbm, k_hbm, v_hbm,
                 xbuf, a_buf, wgu, wqkv, wo_buf, wd_buf, acc_gu, acc_qkv, m_buf, o_buf, k_buf, v_buf,
                 pbuf, precv, rsbuf, ybuf, xown,
                 x_sem, wk_sem, wn_sem, kv_sem, xown_sem, ps_send, ps_recv, rs_send, rs_recv, ag_send, ag_recv,
                 yl_sem, yp_send, yp_recv, credit):
    tokens, width, ff, fpad, q_cols, kv_heads, tp_size = cfg
    blocks = ROW_BLOCKS
    rows = tokens // blocks
    ring = tp_size // 2
    k_w = width // K_STEPS
    n_w = width // N_STEPS
    half = width // 2
    c_w = half // (2 * ring)
    per_n = n_w // c_w
    s_rows = rows // SUBS
    q_local = q_cols // HEAD_DIM
    scale = 1.0 / math.sqrt(HEAD_DIM)
    f32, bf16 = jnp.float32, jnp.bfloat16

    me = lax.axis_index('tp')
    pos, core = me // 2, me % 2
    nxt = (lax.rem(pos + 1, ring) * 2 + core, lax.rem(pos + ring - 1, ring) * 2 + core)
    partner = pos * 2 + (1 - core)
    head_col = pl.multiple_of(me * kv_heads // tp_size * HEAD_DIM, HEAD_DIM)

    barrier = pltpu.get_barrier_semaphore()
    for other in (nxt[0], nxt[1], partner):
        pl.semaphore_signal(barrier, inc=1, device_id={'tp': other}, device_id_type=MESH)
    pl.semaphore_wait(barrier, 3)

    def x_copy(b):
        return pltpu.make_async_copy(x_hbm.at[pl.ds(pl.multiple_of(b * rows, rows), rows)], xbuf, x_sem)

    def k_copies(k):
        s = lax.rem(k, 3)
        lo = pl.multiple_of(k * k_w, k_w)
        return (
            pltpu.make_async_copy(wg_hbm.at[:, pl.ds(lo, k_w)], wgu.at[s, pl.ds(0, ff)], wk_sem.at[s, 0]),
            pltpu.make_async_copy(wu_hbm.at[:, pl.ds(lo, k_w)], wgu.at[s, pl.ds(fpad, ff)], wk_sem.at[s, 1]),
            pltpu.make_async_copy(wq_hbm.at[pl.ds(lo, k_w)], wqkv.at[s, :, pl.ds(0, q_cols)], wk_sem.at[s, 2]),
            pltpu.make_async_copy(wk_hbm.at[pl.ds(lo, k_w), pl.ds(head_col, HEAD_DIM)],
                                  wqkv.at[s, :, pl.ds(q_cols, HEAD_DIM)], wk_sem.at[s, 3]),
            pltpu.make_async_copy(wv_hbm.at[pl.ds(lo, k_w), pl.ds(head_col, HEAD_DIM)],
                                  wqkv.at[s, :, pl.ds(q_cols + HEAD_DIM, HEAD_DIM)], wk_sem.at[s, 4]),
        )

    def n_copies(n):
        s = lax.rem(n, 3)
        piece = n // (N_STEPS // 2)
        side = jnp.where(piece == 0, 1 - core, core)
        lo = pl.multiple_of(side * half + lax.rem(n, N_STEPS // 2) * n_w, n_w)
        return (
            pltpu.make_async_copy(wo_hbm.at[:, pl.ds(lo, n_w)], wo_buf.at[s], wn_sem.at[s, 0]),
            pltpu.make_async_copy(wd_hbm.at[:, pl.ds(lo, n_w)], wd_buf.at[s, pl.ds(0, ff)], wn_sem.at[s, 1]),
        )

    def start(copies):
        for copy in copies:
            copy.start()

    def wait(copies):
        for copy in copies:
            copy.wait()

    def kv_copies(b):
        r = pl.ds(pl.multiple_of(b * rows, rows), rows)
        return (pltpu.make_async_copy(k_buf.at[r], k_hbm.at[r], kv_sem.at[0]),
                pltpu.make_async_copy(v_buf.at[r], v_hbm.at[r], kv_sem.at[1]))

    def xown_copies(b):
        out = []
        for d in range(2):
            col = pl.multiple_of(core * half + (d * ring + pos) * c_w, c_w)
            out.append(pltpu.make_async_copy(
                x_hbm.at[pl.ds(pl.multiple_of(b * rows, rows), rows), pl.ds(col, c_w)],
                xown.at[lax.rem(b, 2), d], xown_sem.at[lax.rem(b, 2), d]))
        return out

    def ps_copy(b, n):
        part = pl.ds(n * per_n, per_n)
        return pltpu.make_async_remote_copy(
            pbuf.at[0, part], precv.at[lax.rem(b, 2), part], ps_send, ps_recv.at[lax.rem(b, 2)],
            device_id={'tp': partner}, device_id_type=MESH)

    def rs_copy(src, b, d, s, sub):
        par = lax.rem(b, 2)
        return pltpu.make_async_remote_copy(
            src, rsbuf.at[par, d, s, sub], rs_send, rs_recv.at[par, d, s, sub],
            device_id={'tp': nxt[d]}, device_id_type=MESH)

    def ag_copy(b, d, s, k, sub):
        ref = ybuf.at[b, d * ring + k, sub_rows(sub)]
        return pltpu.make_async_remote_copy(
            ref, ref, ag_send.at[b], ag_recv.at[b, d, s, sub], device_id={'tp': nxt[d]}, device_id_type=MESH)

    def put_out(b, d, k):
        src = ybuf.at[b, d * ring + k]
        col = pl.multiple_of(core * half + (d * ring + k) * c_w, c_w)
        dst = y_hbm.at[pl.ds(pl.multiple_of(b * rows, rows), rows), pl.ds(col, c_w)]
        pltpu.make_async_copy(src, dst, yl_sem.at[b]).start()
        pltpu.make_async_remote_copy(src, dst, yp_send.at[b], yp_recv.at[b],
                                     device_id={'tp': partner}, device_id_type=MESH).start()

    def sub_rows(sub):
        return pl.ds(pl.multiple_of(sub * s_rows, s_rows), s_rows)

    def own_share(b, d, k, sub):
        par = lax.rem(b, 2)
        q = d * ring + k
        return pbuf[1 + par, q, sub_rows(sub)].astype(f32) + precv[par, q, sub_rows(sub)].astype(f32)

    def rs_step(b, s, sub):
        par = lax.rem(b, 2)
        for d in range(2):
            k = lax.rem(pos + 2 * ring - 1 - s, ring) if d == 0 else lax.rem(pos + 1 + s, ring)

            @pl.when(s == 0)
            def _():
                src = pbuf.at[1 + par, d * ring + k, sub_rows(sub)]
                src[...] = own_share(b, d, k, sub).astype(bf16)
                rs_copy(src, b, d, s, sub).start()

            @pl.when(s > 0)
            def _():
                src = rsbuf.at[par, d, s - 1, sub]
                rs_copy(src, b, d, s - 1, sub).wait_recv()
                src[...] = (own_share(b, d, k, sub) + src[...].astype(f32)).astype(bf16)
                rs_copy(src, b, d, s, sub).start()

    def ag_step(b, s, sub):
        par = lax.rem(b, 2)

        @pl.when((s == 0) & (sub == 0))
        def _():
            wait(xown_copies(b))

        for d in range(2):
            k = lax.rem(pos + ring - s, ring) if d == 0 else lax.rem(pos + s, ring)

            @pl.when(s == 0)
            def _():
                last = rsbuf.at[par, d, ring - 2, sub]
                rs_copy(last, b, d, ring - 2, sub).wait_recv()
                total = own_share(b, d, k, sub) + last[...].astype(f32)
                r = sub_rows(sub)
                ybuf[b, d * ring + k, r] = (xown[par, d, r].astype(f32) + total).astype(bf16)

            @pl.when(s > 0)
            def _():
                ag_copy(b, d, s - 1, k, sub).wait_recv()

            ag_copy(b, d, s, k, sub).start()

            @pl.when(sub == SUBS - 1)
            def _():
                put_out(b, d, k)

    def ag_last(b, sub):
        for d in range(2):
            k = lax.rem(pos + 1, ring) if d == 0 else lax.rem(pos + ring - 1, ring)
            ag_copy(b, d, ring - 2, k, sub).wait_recv()

            @pl.when(sub == SUBS - 1)
            def _():
                put_out(b, d, k)

    def comm(t, j):
        s, sub = j // SUBS, lax.rem(j, SUBS)

        @pl.when((s == 0) & (t >= 3))
        def _():
            ag_last(t - 3, sub)

        @pl.when((t >= 1) & (t <= blocks))
        def _():
            rs_step(t - 1, s, sub)

        @pl.when((t >= 2) & (t <= blocks + 1))
        def _():
            ag_step(t - 2, s, sub)

        @pl.when((j == SUBS) & (t >= 2) & (t < blocks))
        def _():
            pl.semaphore_signal(credit, inc=1, device_id={'tp': partner}, device_id_type=MESH)

    def norm_rows(i, carry=0):
        r = pl.ds(pl.multiple_of(i * 16, 16), 16)
        x32 = xbuf[r].astype(f32)
        inv = lax.rsqrt(jnp.mean(x32 * x32, axis=-1, keepdims=True) + NORM_EPS)
        a_buf[r] = (x32 * inv * g_ref[...].astype(f32)).astype(bf16)
        return carry

    def k_step(t, k):
        s = lax.rem(k, 3)
        wait(k_copies(k))

        @pl.when((k + 2 < K_STEPS) & ((k > 0) | (t > 0)))
        def _():
            start(k_copies(k + 2))

        @pl.when(k + 2 >= K_STEPS)
        def _():
            start(n_copies(k + 2 - K_STEPS))

        a_k = a_buf[:, pl.ds(pl.multiple_of(k * k_w, k_w), k_w)]
        for lo in range(0, 2 * fpad, 512):
            hi = min(lo + 512, 2 * fpad)
            acc_gu[:, lo:hi] += lax.dot_general(a_k, wgu[s, lo:hi], (((1,), (1,)), ((), ())), preferred_element_type=f32)
        acc_qkv[...] += jnp.dot(a_k, wqkv[s], preferred_element_type=f32)

    def rope(v, t):
        r = pl.ds(pl.multiple_of(t * rows, rows), rows)
        return v * cos_ref[r] + pltpu.roll(v, HEAD_DIM // 2, 1) * sin_ref[r]

    def attend(t, h):
        r = pl.ds(pl.multiple_of(t * rows, rows), rows)
        if h == 0:
            k_buf[r] = rope(acc_qkv[:, q_cols:q_cols + HEAD_DIM], t).astype(bf16)
            v_buf[r] = acc_qkv[:, q_cols + HEAD_DIM:q_cols + 2 * HEAD_DIM].astype(bf16)
            start(kv_copies(t))
            start(n_copies(2))
        span = slice(h * HEAD_DIM, (h + 1) * HEAD_DIM)
        q_rot = rope(acc_qkv[:, span], t).astype(bf16)
        scores = lax.dot_general(q_rot, k_buf[...], (((1,), (1,)), ((), ())), preferred_element_type=f32) * scale
        row_id = t * rows + lax.broadcasted_iota(jnp.int32, scores.shape, 0)
        col_id = lax.broadcasted_iota(jnp.int32, scores.shape, 1)
        scores = jnp.where(col_id <= row_id, scores, -1e30)
        expd = jnp.exp(scores - jnp.max(scores, axis=-1, keepdims=True))
        probs = (expd / jnp.sum(expd, axis=-1, keepdims=True)).astype(bf16)
        o_buf[:, span] = jnp.dot(probs, v_buf[...], preferred_element_type=f32).astype(bf16)
        q_rows = rows // q_local
        part = slice(h * q_rows, (h + 1) * q_rows)
        gate = acc_gu[part, 0:fpad]
        m_buf[part] = (gate * (1.0 / (1.0 + jnp.exp(-gate))) * acc_gu[part, fpad:2 * fpad]).astype(bf16)

    def n_step(t, n):
        s = lax.rem(n, 3)
        wait(n_copies(n))

        @pl.when((n >= 1) & (n + 2 < N_STEPS))
        def _():
            start(n_copies(n + 2))

        @pl.when((n + 2 >= N_STEPS) & (t + 1 < blocks))
        def _():
            start(k_copies(n + 2 - N_STEPS))

        @pl.when((n == 0) & (t >= 2))
        def _():
            pl.semaphore_wait(credit, 1)

        @pl.when((n == 0) & (t + 1 < blocks))
        def _():
            x_copy(t + 1).wait()

        mine = n >= N_STEPS // 2
        slot = jnp.where(mine, 1 + lax.rem(t, 2), 0)
        piece = lax.rem(n, N_STEPS // 2)
        for i in range(rows // (16 * N_STEPS)):
            norm_rows(n * (rows // (16 * N_STEPS)) + i)
        o_v, m_v = o_buf[...], m_buf[...]
        for i in range(per_n):
            cols = slice(i * c_w, (i + 1) * c_w)
            out = (jnp.dot(o_v, wo_buf[s, :, cols], preferred_element_type=f32)
                   + jnp.dot(m_v, wd_buf[s, :, cols], preferred_element_type=f32)).astype(bf16)
            pbuf[slot, piece * per_n + i] = out

        @pl.when(jnp.logical_not(mine))
        def _():
            ps_copy(t, piece).start()

    x_copy(0).start()
    wgu[:, ff:fpad] = jnp.zeros((3, fpad - ff, k_w), bf16)
    wgu[:, fpad + ff:] = jnp.zeros((3, fpad - ff, k_w), bf16)
    wd_buf[:, ff:] = jnp.zeros((3, fpad - ff, n_w), bf16)
    k_buf[...] = jnp.zeros(k_buf.shape, bf16)
    v_buf[...] = jnp.zeros(v_buf.shape, bf16)
    x_copy(0).wait()
    for k in range(3):
        start(k_copies(k))
    lax.fori_loop(0, rows // 16, norm_rows, 0)

    def slot_body(t, carry):
        computes = t < blocks
        sends = (t >= 1) & (t <= blocks)

        @pl.when(sends)
        def _():
            pltpu.make_async_copy(precv.at[lax.rem(t - 1, 2)], precv.at[lax.rem(t - 1, 2)],
                                  ps_recv.at[lax.rem(t - 1, 2)]).wait()
            start(xown_copies(t - 1))

        @pl.when(computes)
        def _():
            @pl.when(t + 1 < blocks)
            def _():
                x_copy(t + 1).start()

            acc_gu[...] = jnp.zeros(acc_gu.shape, f32)
            acc_qkv[...] = jnp.zeros(acc_qkv.shape, f32)

        def k_body(k, c):
            comm(t, k)

            @pl.when(computes)
            def _():
                k_step(t, k)
            return c

        lax.fori_loop(0, K_STEPS, k_body, 0)
        for h in range(q_local):
            comm(t, K_STEPS + h)

            @pl.when(computes)
            def _():
                attend(t, h)

        def n_body(n, c):
            comm(t, K_STEPS + q_local + n)

            @pl.when(computes)
            def _():
                n_step(t, n)
            return c

        lax.fori_loop(0, N_STEPS, n_body, 0)

        @pl.when(sends)
        def _():
            pltpu.make_async_copy(rsbuf.at[0], rsbuf.at[0], rs_send).wait()

        @pl.when(computes)
        def _():
            pltpu.make_async_copy(pbuf.at[0], pbuf.at[0], ps_send).wait()
            wait(kv_copies(t))
        return carry

    lax.fori_loop(0, blocks + 2, slot_body, 0)
    for sub in range(SUBS):
        ag_last(blocks - 1, sub)
    for b in range(blocks):
        whole, sent = ybuf.at[b], ybuf.at[b, pl.ds(0, 2 * (ring - 1))]
        pltpu.make_async_copy(sent, sent, ag_send.at[b]).wait()
        for sem in (yl_sem, yp_send, yp_recv):
            pltpu.make_async_copy(whole, whole, sem.at[b]).wait()


def copy_kernel(pieces, y_in, k_in, v_in, y_out, k_out, v_out, y_buf, kv_buf, in_sem, out_sem):
    tokens = y_in.shape[0]
    piece = tokens // pieces
    moves = [(y_in.at[pl.ds(i * piece, piece)], y_buf.at[pl.ds(i * piece, piece)], y_out.at[pl.ds(i * piece, piece)])
             for i in range(pieces)]
    moves += [(k_in, kv_buf.at[0], k_out), (v_in, kv_buf.at[1], v_out)]
    ins = [pltpu.make_async_copy(src, mid, in_sem.at[i]) for i, (src, mid, _) in enumerate(moves)]
    outs = [pltpu.make_async_copy(mid, dst, out_sem.at[i]) for i, (_, mid, dst) in enumerate(moves)]
    for copy in ins:
        copy.start()
    for arrived, leaving in zip(ins, outs):
        arrived.wait()
        leaving.start()
    for copy in outs:
        copy.wait()


def solution(mesh):
    tp_size = mesh.shape['tp']

    def local_layer(x_in, g_norm, w_q, w_k, w_v, w_o, w_gate, w_up, w_down):
        tokens, width = x_in.shape
        ff, q_cols = w_gate.shape[1], w_q.shape[1]
        kv_heads = w_k.shape[1] // HEAD_DIM
        fpad = round_up(ff, HEAD_DIM)
        rows, ring = tokens // ROW_BLOCKS, tp_size // 2
        k_w, n_w = width // K_STEPS, width // N_STEPS
        c_w = width // (4 * ring)
        s_rows = rows // SUBS
        assert rows % (16 * N_STEPS) == 0
        assert K_STEPS + q_cols // HEAD_DIM + N_STEPS == SUBS * (ring - 1)
        cos_full, sin_full = (jnp.asarray(table) for table in rope_tables(tokens))
        cfg = (tokens, width, ff, fpad, q_cols, kv_heads, tp_size)
        bf16, f32 = jnp.bfloat16, jnp.float32
        dma, vmem = pltpu.SemaphoreType.DMA, pltpu.VMEM
        any_spec, vmem_spec = pl.BlockSpec(memory_space=pl.ANY), pl.BlockSpec(memory_space=pltpu.VMEM)
        blocks = ROW_BLOCKS
        y_out, k_out, v_out = pl.pallas_call(
            functools.partial(layer_kernel, cfg),
            out_shape=(jax.ShapeDtypeStruct((tokens, width), bf16),
                       jax.ShapeDtypeStruct((tokens, HEAD_DIM), bf16),
                       jax.ShapeDtypeStruct((tokens, HEAD_DIM), bf16)),
            in_specs=[any_spec, vmem_spec, vmem_spec, vmem_spec] + [any_spec] * 7,
            out_specs=(any_spec,) * 3,
            scratch_shapes=[
                vmem((rows, width), bf16),
                vmem((rows, width), bf16),
                vmem((3, 2 * fpad, k_w), bf16),
                vmem((3, k_w, q_cols + 2 * HEAD_DIM), bf16),
                vmem((3, q_cols, n_w), bf16),
                vmem((3, fpad, n_w), bf16),
                vmem((rows, 2 * fpad), f32),
                vmem((rows, q_cols + 2 * HEAD_DIM), f32),
                vmem((rows, fpad), bf16),
                vmem((rows, q_cols), bf16),
                vmem((tokens, HEAD_DIM), bf16),
                vmem((tokens, HEAD_DIM), bf16),
                vmem((3, 2 * ring, rows, c_w), bf16),
                vmem((2, 2 * ring, rows, c_w), bf16),
                vmem((2, 2, ring - 1, SUBS, s_rows, c_w), bf16),
                vmem((blocks, 2 * ring, rows, c_w), bf16),
                vmem((2, 2, rows, c_w), bf16),
                dma, dma((3, 5)), dma((3, 2)), dma((2,)), dma((2, 2)),
                dma, dma((2,)), dma, dma((2, 2, ring - 1, SUBS)),
                dma((blocks,)), dma((blocks, 2, ring - 1, SUBS)),
                dma((blocks,)), dma((blocks,)), dma((blocks,)),
                pltpu.SemaphoreType.REGULAR,
            ],
            compiler_params=pltpu.CompilerParams(collective_id=0, has_side_effects=True, vmem_limit_bytes=67043328),
        )(x_in, g_norm.reshape(1, width), cos_full, sin_full, w_q, w_k, w_v, w_o, w_gate.T, w_up.T, w_down)
        pieces = 32
        shapes = (y_out, k_out, v_out)
        y_out, k_out, v_out = pl.pallas_call(
            functools.partial(copy_kernel, pieces),
            out_shape=tuple(jax.ShapeDtypeStruct(v.shape, v.dtype) for v in shapes),
            in_specs=[any_spec] * 3,
            out_specs=(any_spec,) * 3,
            scratch_shapes=[vmem((tokens, width), bf16), vmem((2, tokens, HEAD_DIM), bf16),
                            dma((pieces + 2,)), dma((pieces + 2,))],
            compiler_params=pltpu.CompilerParams(vmem_limit_bytes=67043328),
        )(*shapes)
        return y_out, k_out.reshape(tokens, 1, HEAD_DIM), v_out.reshape(tokens, 1, HEAD_DIM)

    return jax.shard_map(local_layer, mesh=mesh, in_specs=(P('dp', None), P(None), P(None, 'tp'), P(None, None), P(None, None), P('tp', None), P(None, 'tp'), P(None, 'tp'), P('tp', None)), out_specs=(P('dp', None), P('dp', 'tp', None), P('dp', 'tp', None)), check_vma=False)
```

```python
import functools
import math
import jax
import jax.numpy as jnp
import numpy as np
from jax import lax
from jax.experimental import pallas as pl
from jax.experimental.pallas import tpu as pltpu
from jax.sharding import PartitionSpec as P

HEAD_DIM = 128
ROPE_BASE = 500000.0
NORM_EPS = 1e-5

ROW_BLOCKS = 4
K_STEPS = 16
N_STEPS = 8
SUBS = 2
MESH = pl.DeviceIdType.MESH


def rope_tables(tokens):
    inv_freq = np.float32(ROPE_BASE) ** (-np.arange(0, HEAD_DIM, 2, dtype=np.float32) / np.float32(HEAD_DIM))
    angles = (np.arange(tokens, dtype=np.float32)[:, None] * inv_freq[None, :].astype(np.float32)).astype(np.float64)
    cos_tab, sin_tab = np.cos(angles).astype(np.float32), np.sin(angles).astype(np.float32)
    return np.concatenate([cos_tab, cos_tab], axis=1), np.concatenate([-sin_tab, sin_tab], axis=1)


def round_up(n, m):
    return (n + m - 1) // m * m


def layer_kernel(cfg, x_hbm, g_ref, cos_ref, sin_ref, wq_hbm, wk_hbm, wv_hbm, wo_hbm, wg_hbm, wu_hbm, wd_hbm,
                 y_hbm, k_hbm, v_hbm,
                 g_row, xbuf, a_buf, wgu, wqkv, wo_buf, wd_buf, acc_gu, acc_qkv, m_buf, o_buf, k_buf, v_buf,
                 pbuf, precv, rsbuf, ybuf, xown,
                 x_sem, wk_sem, wn_sem, kv_sem, xown_sem, ps_send, ps_recv, rs_send, rs_recv, ag_send, ag_recv,
                 yl_sem, yp_send, yp_recv, credit):
    tokens, width, ff, fpad, q_cols, kv_heads, tp_size = cfg
    blocks = ROW_BLOCKS
    rows = tokens // blocks
    ring = tp_size // 2
    k_w = width // K_STEPS
    n_w = width // N_STEPS
    half = width // 2
    c_w = half // (2 * ring)
    per_n = n_w // c_w
    s_rows = rows // SUBS
    stride = (K_STEPS + q_cols // HEAD_DIM + N_STEPS) // (SUBS * (ring - 1))
    q_local = q_cols // HEAD_DIM
    scale = 1.0 / math.sqrt(HEAD_DIM)
    f32, bf16 = jnp.float32, jnp.bfloat16

    me = lax.axis_index('tp')
    pos, core = me // 2, me % 2
    nxt = (lax.rem(pos + 1, ring) * 2 + core, lax.rem(pos + ring - 1, ring) * 2 + core)
    partner = pos * 2 + (1 - core)
    head_col = pl.multiple_of(me * kv_heads // tp_size * HEAD_DIM, HEAD_DIM)

    barrier = pltpu.get_barrier_semaphore()
    for other in (nxt[0], nxt[1], partner):
        pl.semaphore_signal(barrier, inc=1, device_id={'tp': other}, device_id_type=MESH)
    pl.semaphore_wait(barrier, 3)

    def x_copy(b):
        return pltpu.make_async_copy(x_hbm.at[pl.ds(pl.multiple_of(b * rows, rows), rows)], xbuf, x_sem)

    def k_copies(k):
        s = lax.rem(k, 3)
        lo = pl.multiple_of(k * k_w, k_w)
        return (
            pltpu.make_async_copy(wg_hbm.at[:, pl.ds(lo, k_w)], wgu.at[s, pl.ds(0, ff)], wk_sem.at[s, 0]),
            pltpu.make_async_copy(wu_hbm.at[:, pl.ds(lo, k_w)], wgu.at[s, pl.ds(fpad, ff)], wk_sem.at[s, 1]),
            pltpu.make_async_copy(wq_hbm.at[pl.ds(lo, k_w)], wqkv.at[s, :, pl.ds(0, q_cols)], wk_sem.at[s, 2]),
            pltpu.make_async_copy(wk_hbm.at[pl.ds(lo, k_w), pl.ds(head_col, HEAD_DIM)],
                                  wqkv.at[s, :, pl.ds(q_cols, HEAD_DIM)], wk_sem.at[s, 3]),
            pltpu.make_async_copy(wv_hbm.at[pl.ds(lo, k_w), pl.ds(head_col, HEAD_DIM)],
                                  wqkv.at[s, :, pl.ds(q_cols + HEAD_DIM, HEAD_DIM)], wk_sem.at[s, 4]),
        )

    def n_copies(n):
        s = lax.rem(n, 3)
        piece = n // (N_STEPS // 2)
        side = jnp.where(piece == 0, 1 - core, core)
        lo = pl.multiple_of(side * half + lax.rem(n, N_STEPS // 2) * n_w, n_w)
        return (
            pltpu.make_async_copy(wo_hbm.at[:, pl.ds(lo, n_w)], wo_buf.at[s], wn_sem.at[s, 0]),
            pltpu.make_async_copy(wd_hbm.at[:, pl.ds(lo, n_w)], wd_buf.at[s, pl.ds(0, ff)], wn_sem.at[s, 1]),
        )

    def start(copies):
        for copy in copies:
            copy.start()

    def wait(copies):
        for copy in copies:
            copy.wait()

    def kv_copies(b):
        r = pl.ds(pl.multiple_of(b * rows, rows), rows)
        return (pltpu.make_async_copy(k_buf.at[r], k_hbm.at[r], kv_sem.at[0]),
                pltpu.make_async_copy(v_buf.at[r], v_hbm.at[r], kv_sem.at[1]))

    def xown_copies(b):
        out = []
        for d in range(2):
            col = pl.multiple_of(core * half + (d * ring + pos) * c_w, c_w)
            out.append(pltpu.make_async_copy(
                x_hbm.at[pl.ds(pl.multiple_of(b * rows, rows), rows), pl.ds(col, c_w)],
                xown.at[lax.rem(b, 2), d], xown_sem.at[lax.rem(b, 2), d]))
        return out

    def ps_copy(b, n):
        part = pl.ds(n * per_n, per_n)
        return pltpu.make_async_remote_copy(
            pbuf.at[0, part], precv.at[lax.rem(b, 2), part], ps_send, ps_recv.at[lax.rem(b, 2)],
            device_id={'tp': partner}, device_id_type=MESH)

    def rs_copy(src, b, d, s, sub):
        par = lax.rem(b, 2)
        return pltpu.make_async_remote_copy(
            src, rsbuf.at[par, d, s, sub], rs_send, rs_recv.at[par, d, s, sub],
            device_id={'tp': nxt[d]}, device_id_type=MESH)

    def ag_copy(b, d, s, k, sub):
        ref = ybuf.at[b, d * ring + k, sub_rows(sub)]
        return pltpu.make_async_remote_copy(
            ref, ref, ag_send.at[b], ag_recv.at[b, d, s, sub], device_id={'tp': nxt[d]}, device_id_type=MESH)

    def put_out(b, d, k):
        src = ybuf.at[b, d * ring + k]
        col = pl.multiple_of(core * half + (d * ring + k) * c_w, c_w)
        dst = y_hbm.at[pl.ds(pl.multiple_of(b * rows, rows), rows), pl.ds(col, c_w)]
        pltpu.make_async_copy(src, dst, yl_sem.at[b]).start()
        pltpu.make_async_remote_copy(src, dst, yp_send.at[b], yp_recv.at[b],
                                     device_id={'tp': partner}, device_id_type=MESH).start()

    def sub_rows(sub):
        return pl.ds(pl.multiple_of(sub * s_rows, s_rows), s_rows)

    def own_share(b, d, k, sub):
        par = lax.rem(b, 2)
        q = d * ring + k
        return pbuf[1 + par, q, sub_rows(sub)].astype(f32) + precv[par, q, sub_rows(sub)].astype(f32)

    def rs_step(b, s, sub):
        par = lax.rem(b, 2)
        for d in range(2):
            k = lax.rem(pos + 2 * ring - 1 - s, ring) if d == 0 else lax.rem(pos + 1 + s, ring)

            @pl.when(s == 0)
            def _():
                src = pbuf.at[1 + par, d * ring + k, sub_rows(sub)]
                src[...] = own_share(b, d, k, sub).astype(bf16)
                rs_copy(src, b, d, s, sub).start()

            @pl.when(s > 0)
            def _():
                src = rsbuf.at[par, d, s - 1, sub]
                rs_copy(src, b, d, s - 1, sub).wait_recv()
                src[...] = (own_share(b, d, k, sub) + src[...].astype(f32)).astype(bf16)
                rs_copy(src, b, d, s, sub).start()

    def ag_step(b, s, sub):
        par = lax.rem(b, 2)

        @pl.when((s == 0) & (sub == 0))
        def _():
            wait(xown_copies(b))

        for d in range(2):
            k = lax.rem(pos + ring - s, ring) if d == 0 else lax.rem(pos + s, ring)

            @pl.when(s == 0)
            def _():
                last = rsbuf.at[par, d, ring - 2, sub]
                rs_copy(last, b, d, ring - 2, sub).wait_recv()
                total = own_share(b, d, k, sub) + last[...].astype(f32)
                r = sub_rows(sub)
                ybuf[b, d * ring + k, r] = (xown[par, d, r].astype(f32) + total).astype(bf16)

            @pl.when(s > 0)
            def _():
                ag_copy(b, d, s - 1, k, sub).wait_recv()

            ag_copy(b, d, s, k, sub).start()

            @pl.when(sub == SUBS - 1)
            def _():
                put_out(b, d, k)

    def ag_last(b, sub):
        for d in range(2):
            k = lax.rem(pos + 1, ring) if d == 0 else lax.rem(pos + ring - 1, ring)
            ag_copy(b, d, ring - 2, k, sub).wait_recv()

            @pl.when(sub == SUBS - 1)
            def _():
                put_out(b, d, k)

    def comm(t, step):
        if isinstance(step, int):
            if step % stride == 0:
                comm_piece(t, step // stride)
        else:
            @pl.when(lax.rem(step, stride) == 0)
            def _():
                comm_piece(t, step // stride)

    def comm_piece(t, j):
        s, sub = j // SUBS, lax.rem(j, SUBS)

        @pl.when((s == 0) & (t >= 3))
        def _():
            ag_last(t - 3, sub)

        @pl.when((t >= 1) & (t <= blocks))
        def _():
            rs_step(t - 1, s, sub)

        @pl.when((t >= 2) & (t <= blocks + 1))
        def _():
            ag_step(t - 2, s, sub)

        @pl.when((j == SUBS) & (t >= 2) & (t < blocks))
        def _():
            pl.semaphore_signal(credit, inc=1, device_id={'tp': partner}, device_id_type=MESH)

    def norm_rows(i, carry=0):
        r = pl.ds(pl.multiple_of(i * 16, 16), 16)
        x32 = xbuf[r].astype(f32)
        inv = lax.rsqrt(jnp.mean(x32 * x32, axis=-1, keepdims=True) + NORM_EPS)
        a_buf[r] = (x32 * inv * g_row[...]).astype(bf16)
        return carry

    def k_step(t, k):
        s = lax.rem(k, 3)
        wait(k_copies(k))

        @pl.when((k + 2 < K_STEPS) & ((k > 0) | (t > 0)))
        def _():
            start(k_copies(k + 2))

        @pl.when(k + 2 >= K_STEPS)
        def _():
            start(n_copies(k + 2 - K_STEPS))

        a_k = a_buf[:, pl.ds(pl.multiple_of(k * k_w, k_w), k_w)]
        for lo in range(0, 2 * fpad, 512):
            hi = min(lo + 512, 2 * fpad)
            acc_gu[:, lo:hi] += lax.dot_general(a_k, wgu[s, lo:hi], (((1,), (1,)), ((), ())), preferred_element_type=f32)
        acc_qkv[...] += jnp.dot(a_k, wqkv[s], preferred_element_type=f32)

    def rope(v, t):
        r = pl.ds(pl.multiple_of(t * rows, rows), rows)
        return v * cos_ref[r] + pltpu.roll(v, HEAD_DIM // 2, 1) * sin_ref[r]

    def attend(t, h):
        r = pl.ds(pl.multiple_of(t * rows, rows), rows)
        if h == 0:
            k_buf[r] = rope(acc_qkv[:, q_cols:q_cols + HEAD_DIM], t).astype(bf16)
            v_buf[r] = acc_qkv[:, q_cols + HEAD_DIM:q_cols + 2 * HEAD_DIM].astype(bf16)
            start(kv_copies(t))
            start(n_copies(2))
        span = slice(h * HEAD_DIM, (h + 1) * HEAD_DIM)
        q_rot = rope(acc_qkv[:, span], t).astype(bf16)
        scores = lax.dot_general(q_rot, k_buf[...], (((1,), (1,)), ((), ())), preferred_element_type=f32) * scale
        row_id = t * rows + lax.broadcasted_iota(jnp.int32, scores.shape, 0)
        col_id = lax.broadcasted_iota(jnp.int32, scores.shape, 1)
        scores = jnp.where(col_id <= row_id, scores, -1e30)
        expd = jnp.exp(scores - jnp.max(scores, axis=-1, keepdims=True))
        probs = (expd / jnp.sum(expd, axis=-1, keepdims=True)).astype(bf16)
        o_buf[:, span] = jnp.dot(probs, v_buf[...], preferred_element_type=f32).astype(bf16)
        q_rows = rows // q_local
        part = slice(h * q_rows, (h + 1) * q_rows)
        gate = acc_gu[part, 0:fpad]
        m_buf[part] = (gate * (1.0 / (1.0 + jnp.exp(-gate))) * acc_gu[part, fpad:2 * fpad]).astype(bf16)

    def n_step(t, n):
        s = lax.rem(n, 3)
        wait(n_copies(n))

        @pl.when((n >= 1) & (n + 2 < N_STEPS))
        def _():
            start(n_copies(n + 2))

        @pl.when((n + 2 >= N_STEPS) & (t + 1 < blocks))
        def _():
            start(k_copies(n + 2 - N_STEPS))

        @pl.when((n == 0) & (t >= 2))
        def _():
            pl.semaphore_wait(credit, 1)

        @pl.when((n == 0) & (t + 1 < blocks))
        def _():
            x_copy(t + 1).wait()

        mine = n >= N_STEPS // 2
        slot = jnp.where(mine, 1 + lax.rem(t, 2), 0)
        piece = lax.rem(n, N_STEPS // 2)
        for i in range(rows // (16 * N_STEPS)):
            norm_rows(n * (rows // (16 * N_STEPS)) + i)
        o_v, m_v = o_buf[...], m_buf[...]
        for i in range(per_n):
            cols = slice(i * c_w, (i + 1) * c_w)
            out = (jnp.dot(o_v, wo_buf[s, :, cols], preferred_element_type=f32)
                   + jnp.dot(m_v, wd_buf[s, :, cols], preferred_element_type=f32)).astype(bf16)
            pbuf[slot, piece * per_n + i] = out

        @pl.when(jnp.logical_not(mine))
        def _():
            ps_copy(t, piece).start()

    x_copy(0).start()
    gains = g_ref[...].astype(f32)
    for i in range(width // HEAD_DIM):
        g_row[:, i * HEAD_DIM:(i + 1) * HEAD_DIM] = gains[i:i + 1]
    wgu[:, ff:fpad] = jnp.zeros((3, fpad - ff, k_w), bf16)
    wgu[:, fpad + ff:] = jnp.zeros((3, fpad - ff, k_w), bf16)
    wd_buf[:, ff:] = jnp.zeros((3, fpad - ff, n_w), bf16)
    k_buf[...] = jnp.zeros(k_buf.shape, bf16)
    v_buf[...] = jnp.zeros(v_buf.shape, bf16)
    x_copy(0).wait()
    for k in range(3):
        start(k_copies(k))
    lax.fori_loop(0, rows // 16, norm_rows, 0)

    def slot_body(t, carry):
        computes = t < blocks
        sends = (t >= 1) & (t <= blocks)

        @pl.when(sends)
        def _():
            pltpu.make_async_copy(precv.at[lax.rem(t - 1, 2)], precv.at[lax.rem(t - 1, 2)],
                                  ps_recv.at[lax.rem(t - 1, 2)]).wait()
            start(xown_copies(t - 1))

        @pl.when(computes)
        def _():
            @pl.when(t + 1 < blocks)
            def _():
                x_copy(t + 1).start()

            acc_gu[...] = jnp.zeros(acc_gu.shape, f32)
            acc_qkv[...] = jnp.zeros(acc_qkv.shape, f32)

        def k_body(k, c):
            comm(t, k)

            @pl.when(computes)
            def _():
                k_step(t, k)
            return c

        lax.fori_loop(0, K_STEPS, k_body, 0)
        for h in range(q_local):
            comm(t, K_STEPS + h)

            @pl.when(computes)
            def _():
                attend(t, h)

        def n_body(n, c):
            comm(t, K_STEPS + q_local + n)

            @pl.when(computes)
            def _():
                n_step(t, n)
            return c

        lax.fori_loop(0, N_STEPS, n_body, 0)

        @pl.when(sends)
        def _():
            pltpu.make_async_copy(rsbuf.at[0], rsbuf.at[0], rs_send).wait()

        @pl.when(computes)
        def _():
            pltpu.make_async_copy(pbuf.at[0], pbuf.at[0], ps_send).wait()
            wait(kv_copies(t))
        return carry

    lax.fori_loop(0, blocks + 2, slot_body, 0)
    for sub in range(SUBS):
        ag_last(blocks - 1, sub)
    for b in range(blocks):
        whole, sent = ybuf.at[b], ybuf.at[b, pl.ds(0, 2 * (ring - 1))]
        pltpu.make_async_copy(sent, sent, ag_send.at[b]).wait()
        for sem in (yl_sem, yp_send, yp_recv):
            pltpu.make_async_copy(whole, whole, sem.at[b]).wait()


def copy_kernel(pieces, y_in, k_in, v_in, y_out, k_out, v_out, y_buf, kv_buf, in_sem, out_sem):
    tokens = y_in.shape[0]
    piece = tokens // pieces
    moves = [(y_in.at[pl.ds(i * piece, piece)], y_buf.at[pl.ds(i * piece, piece)], y_out.at[pl.ds(i * piece, piece)])
             for i in range(pieces)]
    moves += [(k_in, kv_buf.at[0], k_out), (v_in, kv_buf.at[1], v_out)]
    ins = [pltpu.make_async_copy(src, mid, in_sem.at[i]) for i, (src, mid, _) in enumerate(moves)]
    outs = [pltpu.make_async_copy(mid, dst, out_sem.at[i]) for i, (_, mid, dst) in enumerate(moves)]
    for copy in ins:
        copy.start()
    for arrived, leaving in zip(ins, outs):
        arrived.wait()
        leaving.start()
    for copy in outs:
        copy.wait()


def solution(mesh):
    tp_size = mesh.shape['tp']

    def local_layer(x_in, g_norm, w_q, w_k, w_v, w_o, w_gate, w_up, w_down):
        tokens, width = x_in.shape
        ff, q_cols = w_gate.shape[1], w_q.shape[1]
        kv_heads = w_k.shape[1] // HEAD_DIM
        fpad = round_up(ff, HEAD_DIM)
        rows, ring = tokens // ROW_BLOCKS, tp_size // 2
        k_w, n_w = width // K_STEPS, width // N_STEPS
        c_w = width // (4 * ring)
        s_rows = rows // SUBS
        assert rows % (16 * N_STEPS) == 0
        assert (K_STEPS + q_cols // HEAD_DIM + N_STEPS) % (SUBS * (ring - 1)) == 0
        cos_full, sin_full = (jnp.asarray(table) for table in rope_tables(tokens))
        cfg = (tokens, width, ff, fpad, q_cols, kv_heads, tp_size)
        bf16, f32 = jnp.bfloat16, jnp.float32
        dma, vmem = pltpu.SemaphoreType.DMA, pltpu.VMEM
        any_spec, vmem_spec = pl.BlockSpec(memory_space=pl.ANY), pl.BlockSpec(memory_space=pltpu.VMEM)
        blocks = ROW_BLOCKS
        y_out, k_out, v_out = pl.pallas_call(
            functools.partial(layer_kernel, cfg),
            out_shape=(jax.ShapeDtypeStruct((tokens, width), bf16),
                       jax.ShapeDtypeStruct((tokens, HEAD_DIM), bf16),
                       jax.ShapeDtypeStruct((tokens, HEAD_DIM), bf16)),
            in_specs=[any_spec, vmem_spec, vmem_spec, vmem_spec] + [any_spec] * 7,
            out_specs=(any_spec,) * 3,
            scratch_shapes=[
                vmem((1, width), f32),
                vmem((rows, width), bf16),
                vmem((rows, width), bf16),
                vmem((3, 2 * fpad, k_w), bf16),
                vmem((3, k_w, q_cols + 2 * HEAD_DIM), bf16),
                vmem((3, q_cols, n_w), bf16),
                vmem((3, fpad, n_w), bf16),
                vmem((rows, 2 * fpad), f32),
                vmem((rows, q_cols + 2 * HEAD_DIM), f32),
                vmem((rows, fpad), bf16),
                vmem((rows, q_cols), bf16),
                vmem((tokens, HEAD_DIM), bf16),
                vmem((tokens, HEAD_DIM), bf16),
                vmem((3, 2 * ring, rows, c_w), bf16),
                vmem((2, 2 * ring, rows, c_w), bf16),
                vmem((2, 2, ring - 1, SUBS, s_rows, c_w), bf16),
                vmem((blocks, 2 * ring, rows, c_w), bf16),
                vmem((2, 2, rows, c_w), bf16),
                dma, dma((3, 5)), dma((3, 2)), dma((2,)), dma((2, 2)),
                dma, dma((2,)), dma, dma((2, 2, ring - 1, SUBS)),
                dma((blocks,)), dma((blocks, 2, ring - 1, SUBS)),
                dma((blocks,)), dma((blocks,)), dma((blocks,)),
                pltpu.SemaphoreType.REGULAR,
            ],
            compiler_params=pltpu.CompilerParams(collective_id=0, has_side_effects=True, vmem_limit_bytes=67043328),
        )(x_in, g_norm.reshape(width // HEAD_DIM, HEAD_DIM), cos_full, sin_full, w_q, w_k, w_v, w_o, w_gate.T, w_up.T, w_down)
        pieces = 32
        shapes = (y_out, k_out, v_out)
        y_out, k_out, v_out = pl.pallas_call(
            functools.partial(copy_kernel, pieces),
            out_shape=tuple(jax.ShapeDtypeStruct(v.shape, v.dtype) for v in shapes),
            in_specs=[any_spec] * 3,
            out_specs=(any_spec,) * 3,
            scratch_shapes=[vmem((tokens, width), bf16), vmem((2, tokens, HEAD_DIM), bf16),
                            dma((pieces + 2,)), dma((pieces + 2,))],
            compiler_params=pltpu.CompilerParams(vmem_limit_bytes=67043328),
        )(*shapes)
        return y_out, k_out.reshape(tokens, 1, HEAD_DIM), v_out.reshape(tokens, 1, HEAD_DIM)

    return jax.shard_map(local_layer, mesh=mesh, in_specs=(P('dp', None), P(None), P(None, 'tp'), P(None, None), P(None, None), P('tp', None), P(None, 'tp'), P(None, 'tp'), P('tp', None)), out_specs=(P('dp', None), P('dp', 'tp', None), P('dp', 'tp', None)), check_vma=False)
```
